32 devices in a mesh: dp: 4 (over z), expert: 8 (over y, x, core).
Axes of the slice: x: 2, y: 2, z: 4, core: 2. Of those that a mesh axis runs over, the one named last changes fastest.
Arguments:
- tokens: bfloat16 [2048, 2048], P(('dp', 'expert')), may hold values from -6 to 6
- norm_gain: bfloat16 [2048], replicated, may hold values from 0.099609375 to 1.8984375
- router_weight: bfloat16 [2048, 8], replicated, may hold values from -0.125 to 0.125
- gate_weight: bfloat16 [8, 2048, 5120], P('expert', None, 'dp'), may hold values from -0.125 to 0.125
- up_weight: bfloat16 [8, 2048, 5120], P('expert', None, 'dp'), may hold values from -0.125 to 0.125
- down_weight: bfloat16 [8, 5120, 2048], P('expert', 'dp'), may hold values from -0.078125 to 0.078125
- expert_picks: int32 [4, 8, 128], P('dp'), may hold values from 0 to 511, as said below
- final_gain: bfloat16 [2048], replicated, may hold values from 0.099609375 to 1.8984375
- kv_weight: bfloat16 [2048, 8, 6, 2, 64], P(None, 'expert'), may hold values from -0.125 to 0.125
Outputs:
- moe_out: bfloat16 [2048, 2048], P(('dp', 'expert'))
- kv_cache: bfloat16 [2048, 8, 6, 2, 64], P('dp', 'expert')
The draws below stay inside these ranges and needn't reach their ends.
Inputs may be any that keep to these rules, and one draw needn't show every extreme that they name: `expert_picks`: for each group and expert, 128 different positions in the group. Of the 64 tokens of one device (positions s * 64 to (s + 1) * 64 - 1) one expert picks at most 32, and for every group and expert some device's tokens are picked exactly 32 times.
All inputs are finite; a program needn't handle non-finite values.
Results may differ from the reference program's by a relative error of at most 0.013.
Values may be sent and summed in bfloat16 or wider, within the bound.
No kernel may reach another device: no remote copies, remote signals or barrier semaphores. Data moves between devices by JAX's collectives and lax.ppermute only.
A program may use at most 128 MiB of HBM per device.

```python
import jax
import jax.numpy as jnp
from jax import lax

D = 2048
FF = 5120
DK = 64
TOK_DEV = 64
LAYERS = 6
EXPERTS = 8
HEADS = 8
TOKENS = 2048
CAP = 128
MOST = 32
N_DP = 4
N_EXPERT = 8


def one_expert_picks(sub_key):
    key_full, key_slot, key_perm, key_order = jax.random.split(sub_key, 4)
    full_shard = jax.random.randint(key_full, (), 0, N_EXPERT)
    scores = jax.random.permutation(key_slot, N_EXPERT * MOST).astype(jnp.int32)
    shard_of = jnp.arange(N_EXPERT * MOST, dtype=jnp.int32) // MOST
    scores = jnp.where(shard_of == full_shard, scores - N_EXPERT * MOST, scores)
    chosen = jnp.argsort(scores, stable=True)[:CAP].astype(jnp.int32)
    shard_pos = chosen // MOST
    within = chosen % MOST
    shard_perms = jax.vmap(lambda perm_key: jax.random.permutation(perm_key, TOK_DEV))(jax.random.split(key_perm, N_EXPERT))
    token_pos = shard_pos * TOK_DEV + shard_perms[shard_pos, within].astype(jnp.int32)
    pick_order = jax.random.permutation(key_order, CAP)
    return token_pos[pick_order].astype(jnp.int32)


def draw_expert_picks(key, part):
    base = jax.random.fold_in(key, 7)
    keys = jax.random.split(base, N_DP * EXPERTS)
    all_picks = jax.vmap(one_expert_picks)(keys)
    return all_picks.reshape(N_DP, EXPERTS, CAP).astype(jnp.int32)


def levels(own_key, shape, shards, smallest, high):
    def one(axis_at, parts):
        draws = jax.random.uniform(jax.random.fold_in(jax.random.fold_in(own_key, 6), axis_at), (parts,), jnp.float32, smallest / len(shards), high / len(shards))
        return jnp.repeat(jnp.exp(draws), shape[axis_at] // parts).reshape((-1,) + (1,) * (len(shape) - axis_at - 1))

    level = one(*shards[0])
    for cut in shards[1:]:
        level = level * one(*cut)
    return level


def gaussian(key, dims, scale, bound, cuts=(), kind=jnp.bfloat16):
    level = levels(key, dims, cuts, -0.22, 0.18) if cuts else 1.0
    entries = jax.random.normal(key, dims, jnp.float32) * scale * level
    return jnp.minimum(jnp.maximum(entries, -bound), bound).astype(kind)


def setup_inputs(seed: int = 0) -> dict:
    key_list = jax.random.split(jax.random.key(seed), 10)
    tokens = gaussian(key_list[0], (TOKENS, D), 1.0, 6.0, ((0, 32),))
    norm_gain = jnp.clip(1.0 + 0.18 * jax.random.normal(key_list[1], (D,), jnp.float32), 0.099609375, 1.8984375).astype(jnp.bfloat16)
    router_weight = gaussian(key_list[2], (D, EXPERTS), D ** -0.5, 0.125)
    gate_weight = gaussian(key_list[3], (EXPERTS, D, FF), D ** -0.5, 0.125, ((0, 8), (2, 4)))
    up_weight = gaussian(key_list[4], (EXPERTS, D, FF), D ** -0.5, 0.125, ((0, 8), (2, 4)))
    down_weight = gaussian(key_list[5], (EXPERTS, FF, D), FF ** -0.5, 0.078125, ((0, 8), (1, 4)))
    expert_picks = draw_expert_picks(jax.random.fold_in(key_list[9], 71), 0)
    final_gain = jnp.clip(1.0 + 0.18 * jax.random.normal(key_list[7], (D,), jnp.float32), 0.099609375, 1.8984375).astype(jnp.bfloat16)
    kv_weight = gaussian(key_list[8], (D, HEADS, LAYERS, 2, DK), D ** -0.5, 0.125, ((1, 8),))
    return {"tokens": tokens, "norm_gain": norm_gain, "router_weight": router_weight, "gate_weight": gate_weight, "up_weight": up_weight, "down_weight": down_weight, "expert_picks": expert_picks, "final_gain": final_gain, "kv_weight": kv_weight}


def normalize(values, gain):
    return values * lax.rsqrt(lax.optimization_barrier(jnp.mean(values * values, axis=-1, keepdims=True)) + 1e-06) * gain.astype(jnp.float32)

def reference(tokens, norm_gain, router_weight, gate_weight, up_weight, down_weight, expert_picks, final_gain, kv_weight):
    wide_tokens = tokens.astype(jnp.float32)
    normed = normalize(wide_tokens, norm_gain).astype(jnp.bfloat16)
    gate_probs = jax.nn.sigmoid(jnp.dot(normed, router_weight, preferred_element_type=jnp.float32))
    group_start = jnp.arange(N_DP, dtype=jnp.int32)[:, None, None] * (TOK_DEV * N_EXPERT)
    all_rows = jnp.transpose(group_start + expert_picks, (1, 0, 2)).reshape(EXPERTS, -1).astype(jnp.int32)
    block_width = FF // N_DP

    def one_expert(expert):
        row_index = lax.dynamic_index_in_dim(all_rows, expert, 0, keepdims=False)
        inputs = normed[row_index]
        gate_act = jnp.dot(inputs, gate_weight[expert], preferred_element_type=jnp.float32)
        up_act = jnp.dot(inputs, up_weight[expert], preferred_element_type=jnp.float32)
        hidden = (jax.nn.gelu(gate_act, approximate=True) * up_act).astype(jnp.bfloat16)
        down_here = down_weight[expert]
        total = jnp.zeros((hidden.shape[0], D), jnp.float32)
        for block in range(N_DP):
            partial_sum = jnp.dot(hidden[:, block * block_width:(block + 1) * block_width], down_here[block * block_width:(block + 1) * block_width], preferred_element_type=jnp.float32).astype(jnp.bfloat16)
            partial_sum = lax.optimization_barrier(partial_sum)
            total = total + partial_sum.astype(jnp.float32)
        result = total.astype(jnp.bfloat16)
        weight = gate_probs[row_index, expert]
        return result.astype(jnp.float32) * weight[:, None]
    contributions = lax.map(one_expert, jnp.arange(EXPERTS, dtype=jnp.int32))
    combined = jnp.zeros((TOKENS, D), jnp.float32).at[all_rows.reshape(-1)].add(contributions.reshape(-1, D))
    moe_out = (wide_tokens + combined).astype(jnp.bfloat16)
    encoded = normalize(moe_out.astype(jnp.float32), final_gain).astype(jnp.bfloat16)
    projected = jnp.dot(encoded, kv_weight.reshape(D, -1), preferred_element_type=jnp.float32).astype(jnp.bfloat16)
    kv_cache = projected.reshape(TOKENS, HEADS, LAYERS, 2, DK)
    return (moe_out, kv_cache)
```

```python
import functools

import jax
import jax.numpy as jnp
from jax import lax
from jax.experimental import pallas as pl
from jax.experimental.pallas import tpu as pltpu
from jax.sharding import PartitionSpec as P


def shuffle(value, axis, mask, keep=None):
    size = lax.axis_size(axis)
    pairs = [(i, i ^ mask) for i in range(size) if keep is None or keep(i)]
    return lax.ppermute(value, axis, pairs)


def plane_gather(value):
    size = lax.axis_size("expert")
    blocks = {0: value}
    for mask in range(2, size, 2):
        blocks[mask] = shuffle(value, "expert", mask)
    for mask in range(0, size, 2):
        blocks[mask + 1] = shuffle(blocks[mask], "expert", 1)
    return [blocks[mask] for mask in range(size)]


def select_body(base_ref, picks_ref, gain_ref, *refs):
    blocks, out_ref = refs[:-1], refs[-1]
    rows = blocks[0].shape[0]
    capacity = picks_ref.shape[1]
    column = lax.broadcasted_iota(jnp.int32, (rows, capacity), 0)
    hits = jnp.concatenate(
        [
            (column + base_ref[k] == picks_ref[...]).astype(jnp.bfloat16)
            for k in range(len(blocks))
        ],
        axis=0,
    )
    values = jnp.concatenate([block[...] for block in blocks], axis=0)
    chosen = lax.dot_general(
        hits, values, (((0,), (0,)), ((), ())), preferred_element_type=jnp.float32
    )
    scale = lax.rsqrt(jnp.mean(chosen * chosen, axis=-1, keepdims=True) + 1e-06)
    gain = gain_ref[...].astype(jnp.float32)
    out_ref[...] = (chosen * scale * gain).astype(out_ref.dtype)


def fits(blocks):
    return len(blocks) * blocks[0].size <= 2 * 1024 * 1024


def plain_normalize(wide, gain):
    scale = lax.rsqrt(jnp.mean(wide * wide, axis=-1, keepdims=True) + 1e-06)
    return (wide * scale * gain.astype(jnp.float32)).astype(jnp.bfloat16)


def token_ids(base, rows):
    return (base[:, None] + jnp.arange(rows, dtype=jnp.int32)[None, :]).reshape(-1)


def plain_select(blocks, picks, base, gain):
    ids = token_ids(base, blocks[0].shape[0])
    hits = (picks.reshape(-1, 1) == ids[None, :]).astype(jnp.bfloat16)
    values = jnp.concatenate(blocks, axis=0)
    return plain_normalize(jnp.dot(hits, values, preferred_element_type=jnp.float32), gain)


def plain_prepare(blocks, picks, base, gain, router):
    rows = blocks[0].shape[0]
    all_ids = jnp.arange(len(blocks) * rows, dtype=jnp.int32)
    place = (all_ids[:, None] == token_ids(base, rows)[None, :]).astype(jnp.bfloat16)
    values = jnp.concatenate(blocks, axis=0)
    here = jnp.dot(place, values, preferred_element_type=jnp.float32)
    probs = jax.nn.sigmoid(
        jnp.dot(plain_normalize(here, gain), router, preferred_element_type=jnp.float32)
    )
    hits = all_ids[:, None, None] == picks[None, :, :]
    combine = jnp.where(hits, probs[:, :, None], 0.0).astype(jnp.bfloat16)
    return combine.reshape(all_ids.shape[0], -1), here.astype(jnp.bfloat16)


def plain_finish(blocks, combine, here, own, gain, kv_matrix, rows):
    outputs = jnp.concatenate(blocks, axis=0)
    added = jnp.dot(combine, outputs, preferred_element_type=jnp.float32)
    moe = (here.astype(jnp.float32) + added).astype(jnp.bfloat16)
    encoded = plain_normalize(moe.astype(jnp.float32), gain)
    cache = lax.dot_general(
        kv_matrix, encoded, (((1,), (1,)), ((), ())), preferred_element_type=jnp.float32
    ).astype(jnp.bfloat16)
    return lax.dynamic_slice_in_dim(moe, own * rows, rows, 0), cache


def select(blocks, picks, base, gain):
    if not fits(blocks):
        return plain_select(blocks, picks, base, gain)
    capacity, width = picks.shape[-1], blocks[0].shape[1]
    vmem = pl.BlockSpec(memory_space=pltpu.VMEM)
    return pl.pallas_call(
        select_body,
        in_specs=[pl.BlockSpec(memory_space=pltpu.SMEM)] + [vmem] * (2 + len(blocks)),
        out_specs=vmem,
        out_shape=jax.ShapeDtypeStruct((capacity, width), jnp.bfloat16),
        compiler_params=pltpu.CompilerParams(vmem_limit_bytes=48 * 1024 * 1024),
        name="select",
    )(base, picks.reshape(1, capacity), gain.reshape(1, width), *blocks)


def prepare_body(base_ref, own_ref, picks_ref, gain_ref, router_ref, *refs):
    blocks, (combine_ref, here_ref) = refs[:-2], refs[-2:]
    rows, width = blocks[0].shape
    shards = len(blocks)
    capacity = picks_ref.shape[1]
    gain = gain_ref[...].astype(jnp.float32)
    for k in range(shards):
        wide = blocks[k][...].astype(jnp.float32)
        scale = lax.rsqrt(jnp.mean(wide * wide, axis=-1, keepdims=True) + 1e-06)
        normed = (wide * scale * gain).astype(jnp.bfloat16)
        logits = jnp.dot(normed, router_ref[...], preferred_element_type=jnp.float32)
        probs = jax.nn.sigmoid(logits)
        start = pl.multiple_of(base_ref[k], rows)
        here_ref[pl.ds(start, rows), :] = blocks[k][...]
        ids = lax.broadcasted_iota(jnp.int32, (rows, capacity), 0) + start
        for j in range(shards):
            hit = ids == picks_ref[j : j + 1, :]
            combine_ref[pl.ds(start, rows), j * capacity : (j + 1) * capacity] = (
                jnp.where(hit, probs[:, j : j + 1], 0.0).astype(jnp.bfloat16)
            )


def prepare(blocks, picks, base, own, gain, router):
    if not fits(blocks):
        return plain_prepare(blocks, picks, base, gain, router)
    shards, (rows, width) = len(blocks), blocks[0].shape
    capacity = picks.shape[1]
    vmem = pl.BlockSpec(memory_space=pltpu.VMEM)
    smem = pl.BlockSpec(memory_space=pltpu.SMEM)
    return pl.pallas_call(
        prepare_body,
        in_specs=[smem, smem] + [vmem] * (3 + shards),
        out_specs=[vmem, vmem],
        out_shape=[
            jax.ShapeDtypeStruct((shards * rows, shards * capacity), jnp.bfloat16),
            jax.ShapeDtypeStruct((shards * rows, width), jnp.bfloat16),
        ],
        compiler_params=pltpu.CompilerParams(vmem_limit_bytes=56 * 1024 * 1024),
        name="prepare",
    )(base, own.reshape(1), picks, gain.reshape(1, width), router, *blocks)


def finish_body(own_ref, combine_ref, here_ref, gain_ref, kv_ref, *refs):
    blocks, (moe_ref, cache_ref, all_ref) = refs[:-3], refs[-3:]
    rows = moe_ref.shape[0]
    outputs = jnp.concatenate([block[...] for block in blocks], axis=0)
    added = jnp.dot(combine_ref[...], outputs, preferred_element_type=jnp.float32)
    all_ref[...] = (here_ref[...].astype(jnp.float32) + added).astype(jnp.bfloat16)
    moe_ref[...] = all_ref[pl.ds(pl.multiple_of(own_ref[0] * rows, rows), rows), :]
    wide = all_ref[...].astype(jnp.float32)
    scale = lax.rsqrt(jnp.mean(wide * wide, axis=-1, keepdims=True) + 1e-06)
    encoded = (wide * scale * gain_ref[...].astype(jnp.float32)).astype(jnp.bfloat16)
    cache_ref[...] = lax.dot_general(
        kv_ref[...], encoded, (((1,), (1,)), ((), ())), preferred_element_type=jnp.float32
    ).astype(jnp.bfloat16)


def finish(blocks, combine, here, own, gain, kv_matrix, rows):
    if not fits([here]):
        return plain_finish(blocks, combine, here, own, gain, kv_matrix, rows)
    total, width = here.shape
    vmem = pl.BlockSpec(memory_space=pltpu.VMEM)
    return pl.pallas_call(
        finish_body,
        in_specs=[pl.BlockSpec(memory_space=pltpu.SMEM)] + [vmem] * (4 + len(blocks)),
        out_specs=[vmem, vmem],
        out_shape=[
            jax.ShapeDtypeStruct((rows, width), jnp.bfloat16),
            jax.ShapeDtypeStruct((kv_matrix.shape[0], total), jnp.bfloat16),
        ],
        scratch_shapes=[pltpu.VMEM((total, width), jnp.bfloat16)],
        compiler_params=pltpu.CompilerParams(vmem_limit_bytes=56 * 1024 * 1024),
        name="finish",
    )(own.reshape(1), combine, here, gain.reshape(1, width), kv_matrix, *blocks)


def ffn_body(count, *refs):
    inputs, (gate_ref, up_ref, down_ref) = refs[:count], refs[count : count + 3]
    outputs, (rows_ref, acc_ref) = refs[count + 3 : 2 * count + 3], refs[2 * count + 3 :]
    step = pl.program_id(0)
    size = inputs[0].shape[0]

    @pl.when(step == 0)
    def _():
        for i in range(count):
            rows_ref[i * size : (i + 1) * size, :] = inputs[i][...]

    rows = rows_ref[...]
    gate = jnp.dot(rows, gate_ref[...], preferred_element_type=jnp.float32)
    up = jnp.dot(rows, up_ref[...], preferred_element_type=jnp.float32)
    hidden = (jax.nn.gelu(gate, approximate=True) * up).astype(jnp.bfloat16)
    part = jnp.dot(hidden, down_ref[...], preferred_element_type=jnp.float32)

    @pl.when(step == 0)
    def _():
        acc_ref[...] = part

    @pl.when(step > 0)
    def _():
        acc_ref[...] += part

    @pl.when(step == pl.num_programs(0) - 1)
    def _():
        for i in range(count):
            outputs[i][...] = acc_ref[i * size : (i + 1) * size, :].astype(jnp.bfloat16)


def ffn(inputs, gate_proj, up_proj, down_proj):
    count, (size, width) = len(inputs), inputs[0].shape
    hidden = gate_proj.shape[1]
    tile = 256 if hidden % 256 == 0 else 128
    whole = pl.BlockSpec((size, width), lambda i: (0, 0))
    return pl.pallas_call(
        functools.partial(ffn_body, count),
        grid=(hidden // tile,),
        in_specs=[whole] * count
        + [
            pl.BlockSpec((width, tile), lambda i: (0, i)),
            pl.BlockSpec((width, tile), lambda i: (0, i)),
            pl.BlockSpec((tile, width), lambda i: (i, 0)),
        ],
        out_specs=[whole] * count,
        out_shape=[jax.ShapeDtypeStruct((size, width), jnp.bfloat16)] * count,
        scratch_shapes=[
            pltpu.VMEM((count * size, width), jnp.bfloat16),
            pltpu.VMEM((count * size, width), jnp.float32),
        ],
        compiler_params=pltpu.CompilerParams(
            dimension_semantics=("arbitrary",), vmem_limit_bytes=56 * 1024 * 1024
        ),
        cost_estimate=pl.CostEstimate(
            flops=6 * count * size * width * hidden,
            bytes_accessed=6 * width * hidden + 4 * count * size * width,
            transcendentals=count * size * hidden,
        ),
        name="ffn",
    )(*inputs, gate_proj, up_proj, down_proj)


def local(
    tokens,
    norm_gain,
    router_weight,
    gate_weight,
    up_weight,
    down_weight,
    expert_picks,
    final_gain,
    kv_weight,
):
    shards = lax.axis_size("expert")
    groups = lax.axis_size("dp")
    own = lax.axis_index("expert")
    tok_rows, width = tokens.shape
    group_rows = shards * tok_rows
    capacity = expert_picks.shape[2]
    order = jnp.arange(shards, dtype=jnp.int32) ^ own
    base = order * tok_rows
    picks = expert_picks[0][order]
    weights = (gate_weight[0], up_weight[0], down_weight[0])

    dense = fits([tokens] * shards)
    far = {
        mask: (shuffle(tokens, "dp", mask), shuffle(picks[:1], "dp", mask))
        for mask in range(groups - 1, 1, -1)
        if dense
    }
    blocks = plane_gather(tokens)
    inputs = {0: select(blocks, picks[0], base, norm_gain)}
    for mask in range(1, groups):
        if mask not in far:
            inputs[mask] = shuffle(inputs[0], "dp", mask)
    for mask, (spread, rows) in far.items():
        inputs[mask] = select(plane_gather(spread), rows, base, norm_gain)
    combine, here = prepare(blocks, picks, base, own, norm_gain, router_weight[:, order])

    parts = {}
    sequence = [0] + list(range(groups - 1, 0, -1))
    half = max(groups // 2, 1)
    for start in range(0, groups, half):
        batch = sequence[start : start + half]
        result = ffn([inputs[mask] for mask in batch], *weights)
        for i, mask in enumerate(batch):
            parts[mask] = result[i]
    total = parts[0].astype(jnp.float32)
    for mask in range(groups - 1, 0, -1):
        total += shuffle(parts[mask], "dp", mask).astype(jnp.float32)
    returned = plane_gather(total.astype(jnp.bfloat16))
    kv_matrix = kv_weight.reshape(width, -1).T
    moe_out, kv_rows = finish(returned, combine, here, own, final_gain, kv_matrix, tok_rows)
    kv_cache = kv_rows.T.reshape((group_rows,) + kv_weight.shape[1:])
    return (moe_out, kv_cache)


def solution(mesh):
    in_specs = (
        P(("dp", "expert"), None),
        P(),
        P(),
        P("expert", None, "dp"),
        P("expert", None, "dp"),
        P("expert", "dp", None),
        P("dp", None, None),
        P(),
        P(None, "expert", None, None, None),
    )
    out_specs = (P(("dp", "expert"), None), P("dp", "expert", None, None, None))
    return jax.shard_map(local, mesh=mesh, in_specs=in_specs, out_specs=out_specs, check_vma=False)
```

```python
import functools

import jax
import jax.numpy as jnp
from jax import lax
from jax.experimental import pallas as pl
from jax.experimental.pallas import tpu as pltpu
from jax.sharding import PartitionSpec as P


def shuffle(value, axis, mask):
    size = lax.axis_size(axis)
    return lax.ppermute(value, axis, [(i, i ^ mask) for i in range(size)])


def plane_gather(value):
    size = lax.axis_size("expert")
    blocks = {0: value}
    for mask in range(2, size, 2):
        blocks[mask] = shuffle(value, "expert", mask)
    for mask in range(0, size, 2):
        blocks[mask + 1] = shuffle(blocks[mask], "expert", 1)
    return [blocks[mask] for mask in range(size)]


def select_body(base_ref, picks_ref, gain_ref, *refs):
    blocks, out_ref = refs[:-1], refs[-1]
    rows = blocks[0].shape[0]
    capacity = picks_ref.shape[1]
    column = lax.broadcasted_iota(jnp.int32, (rows, capacity), 0)
    hits = jnp.concatenate(
        [
            (column + base_ref[k] == picks_ref[...]).astype(jnp.bfloat16)
            for k in range(len(blocks))
        ],
        axis=0,
    )
    values = jnp.concatenate([block[...] for block in blocks], axis=0)
    chosen = lax.dot_general(
        hits, values, (((0,), (0,)), ((), ())), preferred_element_type=jnp.float32
    )
    scale = lax.rsqrt(jnp.mean(chosen * chosen, axis=-1, keepdims=True) + 1e-06)
    gain = gain_ref[...].astype(jnp.float32)
    out_ref[...] = (chosen * scale * gain).astype(out_ref.dtype)


def fits(blocks):
    return len(blocks) * blocks[0].size <= 2 * 1024 * 1024


def plain_normalize(wide, gain):
    scale = lax.rsqrt(jnp.mean(wide * wide, axis=-1, keepdims=True) + 1e-06)
    return (wide * scale * gain.astype(jnp.float32)).astype(jnp.bfloat16)


def token_ids(base, rows):
    return (base[:, None] + jnp.arange(rows, dtype=jnp.int32)[None, :]).reshape(-1)


def plain_select(blocks, picks, base, gain):
    ids = token_ids(base, blocks[0].shape[0])
    hits = (picks.reshape(-1, 1) == ids[None, :]).astype(jnp.bfloat16)
    values = jnp.concatenate(blocks, axis=0)
    return plain_normalize(jnp.dot(hits, values, preferred_element_type=jnp.float32), gain)


def plain_prepare(blocks, picks, base, gain, router):
    rows = blocks[0].shape[0]
    all_ids = jnp.arange(len(blocks) * rows, dtype=jnp.int32)
    place = (all_ids[:, None] == token_ids(base, rows)[None, :]).astype(jnp.bfloat16)
    values = jnp.concatenate(blocks, axis=0)
    here = jnp.dot(place, values, preferred_element_type=jnp.float32)
    probs = jax.nn.sigmoid(
        jnp.dot(plain_normalize(here, gain), router, preferred_element_type=jnp.float32)
    )
    hits = all_ids[:, None, None] == picks[None, :, :]
    combine = jnp.where(hits, probs[:, :, None], 0.0).astype(jnp.bfloat16)
    return combine.reshape(all_ids.shape[0], -1), here.astype(jnp.bfloat16)


def plain_finish(blocks, combine, here, own, gain, kv_matrix, rows):
    outputs = jnp.concatenate(blocks, axis=0)
    added = jnp.dot(combine, outputs, preferred_element_type=jnp.float32)
    moe = (here.astype(jnp.float32) + added).astype(jnp.bfloat16)
    encoded = plain_normalize(moe.astype(jnp.float32), gain)
    cache = lax.dot_general(
        kv_matrix, encoded, (((1,), (1,)), ((), ())), preferred_element_type=jnp.float32
    ).astype(jnp.bfloat16)
    return lax.dynamic_slice_in_dim(moe, own * rows, rows, 0), cache


def select(blocks, picks, base, gain):
    if not fits(blocks):
        return plain_select(blocks, picks, base, gain)
    capacity, width = picks.shape[-1], blocks[0].shape[1]
    vmem = pl.BlockSpec(memory_space=pltpu.VMEM)
    return pl.pallas_call(
        select_body,
        in_specs=[pl.BlockSpec(memory_space=pltpu.SMEM)] + [vmem] * (2 + len(blocks)),
        out_specs=vmem,
        out_shape=jax.ShapeDtypeStruct((capacity, width), jnp.bfloat16),
        compiler_params=pltpu.CompilerParams(vmem_limit_bytes=48 * 1024 * 1024),
        name="select",
    )(base, picks.reshape(1, capacity), gain.reshape(1, width), *blocks)


def prepare_body(base_ref, own_ref, picks_ref, gain_ref, router_ref, *refs):
    blocks, (combine_ref, here_ref) = refs[:-2], refs[-2:]
    rows, _ = blocks[0].shape
    shards = len(blocks)
    capacity = picks_ref.shape[1]
    gain = gain_ref[...].astype(jnp.float32)
    for k in range(shards):
        wide = blocks[k][...].astype(jnp.float32)
        scale = lax.rsqrt(jnp.mean(wide * wide, axis=-1, keepdims=True) + 1e-06)
        normed = (wide * scale * gain).astype(jnp.bfloat16)
        logits = jnp.dot(normed, router_ref[...], preferred_element_type=jnp.float32)
        probs = jax.nn.sigmoid(logits)
        start = pl.multiple_of(base_ref[k], rows)
        here_ref[pl.ds(start, rows), :] = blocks[k][...]
        ids = lax.broadcasted_iota(jnp.int32, (rows, capacity), 0) + start
        for j in range(shards):
            hit = ids == picks_ref[j : j + 1, :]
            combine_ref[pl.ds(start, rows), j * capacity : (j + 1) * capacity] = (
                jnp.where(hit, probs[:, j : j + 1], 0.0).astype(jnp.bfloat16)
            )


def prepare(blocks, picks, base, own, gain, router):
    if not fits(blocks):
        return plain_prepare(blocks, picks, base, gain, router)
    shards, (rows, width) = len(blocks), blocks[0].shape
    capacity = picks.shape[1]
    vmem = pl.BlockSpec(memory_space=pltpu.VMEM)
    smem = pl.BlockSpec(memory_space=pltpu.SMEM)
    return pl.pallas_call(
        prepare_body,
        in_specs=[smem, smem] + [vmem] * (3 + shards),
        out_specs=[vmem, vmem],
        out_shape=[
            jax.ShapeDtypeStruct((shards * rows, shards * capacity), jnp.bfloat16),
            jax.ShapeDtypeStruct((shards * rows, width), jnp.bfloat16),
        ],
        compiler_params=pltpu.CompilerParams(vmem_limit_bytes=56 * 1024 * 1024),
        name="prepare",
    )(base, own.reshape(1), picks, gain.reshape(1, width), router, *blocks)


def finish_body(stage, stages, shards, *refs):
    own_ref, combine_hbm, here_hbm, gain_ref, kv_hbm = refs[:5]
    blocks, refs = refs[5 : 5 + shards], refs[5 + shards :]
    first, last = stage == 0, stage == stages - 1
    if not first:
        (square_hbm, cache_hbm, *before), refs = refs[: 2 + stage], refs[2 + stage :]
    outs, (combine_ref, here_ref, kv_ref, output_ref, square_ref, cache_ref, sem) = (
        refs[:-7],
        refs[-7:],
    )
    capacity, piece = blocks[0].shape
    span = slice(stage * piece, (stage + 1) * piece)
    copies = [pltpu.make_async_copy(combine_hbm, combine_ref, sem.at[0])]
    for k in range(shards):
        place = output_ref.at[k * capacity : (k + 1) * capacity, :]
        copies.append(pltpu.make_async_copy(blocks[k], place, sem.at[1 + k]))
    copies.append(
        pltpu.make_async_copy(here_hbm.at[:, span], here_ref, sem.at[shards + 1])
    )
    late = [pltpu.make_async_copy(kv_hbm.at[:, span], kv_ref, sem.at[shards + 2])]
    if not first:
        late.append(pltpu.make_async_copy(square_hbm, square_ref, sem.at[shards + 3]))
        late.append(pltpu.make_async_copy(cache_hbm, cache_ref, sem.at[shards + 4]))
    for copy in copies + late:
        copy.start()
    for copy in copies:
        copy.wait()
    added = jnp.dot(combine_ref[...], output_ref[...], preferred_element_type=jnp.float32)
    here_ref[...] = (here_ref[...].astype(jnp.float32) + added).astype(jnp.bfloat16)
    rows = outs[0].shape[0]
    mine = here_ref[pl.ds(pl.multiple_of(own_ref[0] * rows, rows), rows), :]
    if last:
        for j in range(stage):
            outs[0][:, j * piece : (j + 1) * piece] = before[j][...]
        outs[0][:, span] = mine
    else:
        outs[0][...] = mine
    wide = here_ref[...].astype(jnp.float32)
    scaled = (wide * gain_ref[:, span].astype(jnp.float32)).astype(jnp.bfloat16)
    square = jnp.sum(wide * wide, axis=-1, keepdims=True)
    for copy in late:
        copy.wait()
    cache = lax.dot_general(
        kv_ref[...], scaled, (((1,), (1,)), ((), ())), preferred_element_type=jnp.float32
    )
    if not first:
        cache = cache + cache_ref[...]
        square = square + square_ref[...]
    square = jnp.broadcast_to(square, square_ref.shape)
    if last:
        scale = lax.rsqrt(square / (piece * stages) + 1e-06)
        outs[1][...] = (cache * jnp.transpose(scale)[0:1, :]).astype(jnp.bfloat16)
    else:
        outs[1][...] = square
        outs[2][...] = cache


def finish(stage, stages, blocks, combine, here, own, gain, kv_matrix, rows, state):
    (total, width), (capacity, piece) = here.shape, blocks[0].shape
    heads = kv_matrix.shape[0]
    vmem = pl.BlockSpec(memory_space=pltpu.VMEM)
    hbm = pl.BlockSpec(memory_space=pl.ANY)
    shards = len(blocks)
    if stage == stages - 1:
        shapes = [((rows, width), jnp.bfloat16), ((heads, total), jnp.bfloat16)]
    else:
        shapes = [
            ((rows, piece), jnp.bfloat16),
            ((total, 128), jnp.float32),
            ((heads, total), jnp.float32),
        ]
    specs = [pl.BlockSpec(memory_space=pltpu.SMEM), hbm, hbm, vmem, hbm]
    specs += [hbm] * shards + [hbm] * min(len(state), 2) + [vmem] * max(len(state) - 2, 0)
    return pl.pallas_call(
        functools.partial(finish_body, stage, stages, shards),
        in_specs=specs,
        out_specs=[vmem] * len(shapes),
        out_shape=[jax.ShapeDtypeStruct(*shape) for shape in shapes],
        scratch_shapes=[
            pltpu.VMEM(combine.shape, jnp.bfloat16),
            pltpu.VMEM((total, piece), jnp.bfloat16),
            pltpu.VMEM((heads, piece), jnp.bfloat16),
            pltpu.VMEM((shards * capacity, piece), jnp.bfloat16),
            pltpu.VMEM((total, 128), jnp.float32),
            pltpu.VMEM((heads, total), jnp.float32),
            pltpu.SemaphoreType.DMA((shards + 5,)),
        ],
        compiler_params=pltpu.CompilerParams(vmem_limit_bytes=56 * 1024 * 1024),
        name="finish",
    )(own.reshape(1), combine, here, gain.reshape(1, width), kv_matrix, *blocks, *state)


def ffn_body(count, tile, pieces, *refs):
    inputs, weights = refs[:count], refs[count : count + 3]
    outputs = refs[count + 3 : count + 3 + sum(pieces)]
    rest = refs[count + 3 + sum(pieces) :]
    held, (rows_ref, acc_ref, sem) = rest[:3], rest[3:]
    size, width = inputs[0].shape
    steps = weights[0].shape[1] // tile
    loads = []
    for i in range(steps):
        span = slice(i * tile, (i + 1) * tile)
        places = [(slice(None), span), (slice(None), span), (span, slice(None))]
        loads.append(
            [
                pltpu.make_async_copy(
                    weights[k].at[place], held[k].at[place], sem.at[3 * i + k]
                )
                for k, place in enumerate(places)
            ]
        )
    ahead = min(2, steps)
    for copy in sum(loads[:ahead], []):
        copy.start()
    for i in range(count):
        rows_ref[i * size : (i + 1) * size, :] = inputs[i][...]
    for i in range(steps):
        span = slice(i * tile, (i + 1) * tile)
        for copy in loads[i]:
            copy.wait()
        for copy in loads[i + ahead] if i + ahead < steps else []:
            copy.start()
        rows = rows_ref[...]
        gate = jnp.dot(rows, held[0][:, span], preferred_element_type=jnp.float32)
        up = jnp.dot(rows, held[1][:, span], preferred_element_type=jnp.float32)
        hidden = (jax.nn.gelu(gate, approximate=True) * up).astype(jnp.bfloat16)
        part = jnp.dot(hidden, held[2][span, :], preferred_element_type=jnp.float32)
        if i > 0:
            part = acc_ref[...] + part
        if i < steps - 1:
            acc_ref[...] = part
    at = 0
    for i in range(count):
        piece = width // pieces[i]
        for j in range(pieces[i]):
            block = part[i * size : (i + 1) * size, j * piece : (j + 1) * piece]
            outputs[at][...] = block.astype(jnp.bfloat16)
            at += 1


def ffn(inputs, weights, pieces):
    count, (size, width) = len(inputs), inputs[0].shape
    hidden = weights[0].shape[1]
    tile = 256 if hidden % 256 == 0 else 128
    vmem = pl.BlockSpec(memory_space=pltpu.VMEM)
    shapes = [
        jax.ShapeDtypeStruct((size, width // parts), jnp.bfloat16)
        for parts in pieces
        for _ in range(parts)
    ]
    flat = pl.pallas_call(
        functools.partial(ffn_body, count, tile, pieces),
        in_specs=[vmem] * count + [pl.BlockSpec(memory_space=pl.ANY)] * 3,
        out_specs=[vmem] * len(shapes),
        out_shape=shapes,
        scratch_shapes=[
            pltpu.VMEM((width, hidden), jnp.bfloat16),
            pltpu.VMEM((width, hidden), jnp.bfloat16),
            pltpu.VMEM((hidden, width), jnp.bfloat16),
            pltpu.VMEM((count * size, width), jnp.bfloat16),
            pltpu.VMEM((count * size, width), jnp.float32),
            pltpu.SemaphoreType.DMA((3 * (hidden // tile),)),
        ],
        compiler_params=pltpu.CompilerParams(vmem_limit_bytes=56 * 1024 * 1024),
        cost_estimate=pl.CostEstimate(
            flops=6 * count * size * width * hidden,
            bytes_accessed=6 * width * hidden + 4 * count * size * width,
            transcendentals=count * size * hidden,
        ),
        name="ffn",
    )(*inputs, *weights)
    flat = list(flat)
    return [[flat.pop(0) for _ in range(parts)] for parts in pieces]


def local(
    tokens,
    norm_gain,
    router_weight,
    gate_weight,
    up_weight,
    down_weight,
    expert_picks,
    final_gain,
    kv_weight,
):
    shards = lax.axis_size("expert")
    groups = lax.axis_size("dp")
    own = lax.axis_index("expert")
    tok_rows, width = tokens.shape
    group_rows = shards * tok_rows
    order = jnp.arange(shards, dtype=jnp.int32) ^ own
    base = order * tok_rows
    picks = expert_picks[0][order]
    weights = (gate_weight[0], up_weight[0], down_weight[0])

    dense = fits([tokens] * shards)
    own_picks = lax.dynamic_slice_in_dim(expert_picks[0], own, 1, 0)
    far = {
        mask: (shuffle(tokens, "dp", mask), shuffle(own_picks, "dp", mask))
        for mask in range(groups - 1, 1, -1)
        if dense
    }
    blocks = plane_gather(tokens)
    inputs = {0: select(blocks, own_picks, base, norm_gain)}
    for mask in range(1, groups):
        if mask not in far:
            inputs[mask] = shuffle(inputs[0], "dp", mask)
    for mask, (spread, rows) in far.items():
        gathered = plane_gather(spread)
        inputs[mask] = select(gathered, rows, base, norm_gain)
    combine, here = prepare(
        blocks, picks, base, own, norm_gain, router_weight[:, order]
    )

    stages = 2 if dense else 1
    piece = width // stages
    split = lambda mask: stages if mask == 2 and dense else 1
    parts = {}
    sequence = [0] + list(range(groups - 1, 0, -1))
    half = max(groups // 2, 1)
    for start in range(0, groups, half):
        batch = sequence[start : start + half]
        result = ffn([inputs[m] for m in batch], weights, [split(m) for m in batch])
        parts.update(zip(batch, result))
    received = {
        mask: [shuffle(value, "dp", mask) for value in parts[mask]]
        for mask in range(1, groups)
    }
    received[0] = parts[0]
    kv_matrix = kv_weight.reshape(width, -1).T
    state = []
    for stage in range(stages):
        total = 0.0
        for mask in sequence:
            values = received[mask]
            if len(values) == stages:
                value = values[stage]
            else:
                value = values[0][:, stage * piece : (stage + 1) * piece]
            if stage > 0:
                value, _ = lax.optimization_barrier((value, summed))
            total += value.astype(jnp.float32)
        summed = total.astype(jnp.bfloat16)
        returned = plane_gather(summed)
        if not dense:
            moe_out, kv_rows = plain_finish(
                returned, combine, here, own, final_gain, kv_matrix, tok_rows
            )
            continue
        result = finish(
            stage, stages, returned, combine, here, own, final_gain, kv_matrix, tok_rows, state
        )
        if stage == stages - 1:
            moe_out, kv_rows = result
        else:
            state = [result[1], result[2]] + state[2:] + [result[0]]
    kv_cache = kv_rows.T.reshape((group_rows,) + kv_weight.shape[1:])
    return (moe_out, kv_cache)


def solution(mesh):
    in_specs = (
        P(("dp", "expert"), None),
        P(),
        P(),
        P("expert", None, "dp"),
        P("expert", None, "dp"),
        P("expert", "dp", None),
        P("dp", None, None),
        P(),
        P(None, "expert", None, None, None),
    )
    out_specs = (P(("dp", "expert"), None), P("dp", "expert", None, None, None))

    return jax.shard_map(local, mesh=mesh, in_specs=in_specs, out_specs=out_specs, check_vma=False)
```

```python
import functools

import jax
import jax.numpy as jnp
from jax import lax
from jax.experimental import pallas as pl
from jax.experimental.pallas import tpu as pltpu
from jax.sharding import PartitionSpec as P


def shuffle(value, axis, mask, keep=lambda i: True):
    size = lax.axis_size(axis)
    return lax.ppermute(value, axis, [(i, i ^ mask) for i in range(size) if keep(i)])


def plane_gather(value):
    size = lax.axis_size("expert")
    blocks = {0: value}
    for mask in range(2, size, 2):
        blocks[mask] = shuffle(value, "expert", mask)
    for mask in range(0, size, 2):
        blocks[mask + 1] = shuffle(blocks[mask], "expert", 1)
    return [blocks[mask] for mask in range(size)]


def select_body(base_ref, picks_ref, gain_ref, *refs):
    blocks, out_ref = refs[:-1], refs[-1]
    rows = blocks[0].shape[0]
    capacity = picks_ref.shape[1]
    column = lax.broadcasted_iota(jnp.int32, (rows, capacity), 0)
    hits = jnp.concatenate(
        [
            (column + base_ref[k] == picks_ref[...]).astype(jnp.bfloat16)
            for k in range(len(blocks))
        ],
        axis=0,
    )
    values = jnp.concatenate([block[...] for block in blocks], axis=0)
    chosen = lax.dot_general(
        hits, values, (((0,), (0,)), ((), ())), preferred_element_type=jnp.float32
    )
    scale = lax.rsqrt(jnp.mean(chosen * chosen, axis=-1, keepdims=True) + 1e-06)
    gain = gain_ref[...].astype(jnp.float32)
    out_ref[...] = (chosen * scale * gain).astype(out_ref.dtype)


def fits(blocks):
    return len(blocks) * blocks[0].size <= 2 * 1024 * 1024


def plain_normalize(wide, gain):
    scale = lax.rsqrt(jnp.mean(wide * wide, axis=-1, keepdims=True) + 1e-06)
    return (wide * scale * gain.astype(jnp.float32)).astype(jnp.bfloat16)


def token_ids(base, rows):
    return (base[:, None] + jnp.arange(rows, dtype=jnp.int32)[None, :]).reshape(-1)


def plain_select(blocks, picks, base, gain):
    ids = token_ids(base, blocks[0].shape[0])
    hits = (picks.reshape(-1, 1) == ids[None, :]).astype(jnp.bfloat16)
    values = jnp.concatenate(blocks, axis=0)
    return plain_normalize(jnp.dot(hits, values, preferred_element_type=jnp.float32), gain)


def plain_prepare(blocks, picks, base, gain, router):
    rows = blocks[0].shape[0]
    all_ids = jnp.arange(len(blocks) * rows, dtype=jnp.int32)
    place = (all_ids[:, None] == token_ids(base, rows)[None, :]).astype(jnp.bfloat16)
    values = jnp.concatenate(blocks, axis=0)
    here = jnp.dot(place, values, preferred_element_type=jnp.float32)
    probs = jax.nn.sigmoid(
        jnp.dot(plain_normalize(here, gain), router, preferred_element_type=jnp.float32)
    )
    hits = all_ids[:, None, None] == picks[None, :, :]
    combine = jnp.where(hits, probs[:, :, None], 0.0).astype(jnp.bfloat16)
    return combine.reshape(all_ids.shape[0], -1), here.astype(jnp.bfloat16)


def plain_finish(blocks, combine, here, own, gain, kv_matrix, rows):
    outputs = jnp.concatenate(blocks, axis=0)
    added = jnp.dot(combine, outputs, preferred_element_type=jnp.float32)
    moe = (here.astype(jnp.float32) + added).astype(jnp.bfloat16)
    encoded = plain_normalize(moe.astype(jnp.float32), gain)
    cache = lax.dot_general(
        kv_matrix, encoded, (((1,), (1,)), ((), ())), preferred_element_type=jnp.float32
    ).astype(jnp.bfloat16)
    return lax.dynamic_slice_in_dim(moe, own * rows, rows, 0), cache


def select(blocks, picks, base, gain):
    if not fits(blocks):
        return plain_select(blocks, picks, base, gain)
    capacity, width = picks.shape[-1], blocks[0].shape[1]
    vmem = pl.BlockSpec(memory_space=pltpu.VMEM)
    return pl.pallas_call(
        select_body,
        in_specs=[pl.BlockSpec(memory_space=pltpu.SMEM)] + [vmem] * (2 + len(blocks)),
        out_specs=vmem,
        out_shape=jax.ShapeDtypeStruct((capacity, width), jnp.bfloat16),
        compiler_params=pltpu.CompilerParams(vmem_limit_bytes=12 * 1024 * 1024),
        name="select",
    )(base, picks.reshape(1, capacity), gain.reshape(1, width), *blocks)


def prepare_body(base_ref, own_ref, picks_ref, gain_ref, router_ref, *refs):
    blocks, (combine_ref, here_ref) = refs[:-2], refs[-2:]
    rows, _ = blocks[0].shape
    shards = len(blocks)
    capacity = picks_ref.shape[1]
    gain = gain_ref[...].astype(jnp.float32)
    for k in range(shards):
        wide = blocks[k][...].astype(jnp.float32)
        scale = lax.rsqrt(jnp.mean(wide * wide, axis=-1, keepdims=True) + 1e-06)
        normed = (wide * scale * gain).astype(jnp.bfloat16)
        logits = jnp.dot(normed, router_ref[...], preferred_element_type=jnp.float32)
        probs = jax.nn.sigmoid(logits)
        start = pl.multiple_of(base_ref[k], rows)
        here_ref[pl.ds(start, rows), :] = blocks[k][...]
        ids = lax.broadcasted_iota(jnp.int32, (rows, capacity), 0) + start
        for j in range(shards):
            hit = ids == picks_ref[j : j + 1, :]
            combine_ref[pl.ds(start, rows), j * capacity : (j + 1) * capacity] = (
                jnp.where(hit, probs[:, j : j + 1], 0.0).astype(jnp.bfloat16)
            )


def prepare(blocks, picks, base, own, gain, router):
    if not fits(blocks):
        return plain_prepare(blocks, picks, base, gain, router)
    shards, (rows, width) = len(blocks), blocks[0].shape
    capacity = picks.shape[1]
    vmem = pl.BlockSpec(memory_space=pltpu.VMEM)
    smem = pl.BlockSpec(memory_space=pltpu.SMEM)
    return pl.pallas_call(
        prepare_body,
        in_specs=[smem, smem] + [vmem] * (3 + shards),
        out_specs=[vmem, vmem],
        out_shape=[
            jax.ShapeDtypeStruct((shards * rows, shards * capacity), jnp.bfloat16),
            jax.ShapeDtypeStruct((shards * rows, width), jnp.bfloat16),
        ],
        compiler_params=pltpu.CompilerParams(vmem_limit_bytes=24 * 1024 * 1024),
        name="prepare",
    )(base, own.reshape(1), picks, gain.reshape(1, width), router, *blocks)


def finish_body(stage, stages, shards, *refs):
    own_ref, combine_hbm, here_hbm, gain_ref, kv_hbm = refs[:5]
    blocks, refs = refs[5 : 5 + shards], refs[5 + shards :]
    first, last = stage == 0, stage == stages - 1
    if not first:
        (square_hbm, cache_hbm, *before), refs = refs[: 2 + stage], refs[2 + stage :]
    outs, (combine_ref, here_ref, kv_ref, output_ref, square_ref, cache_ref, sem) = (
        refs[:-7],
        refs[-7:],
    )
    capacity, piece = blocks[0].shape
    span = slice(stage * piece, (stage + 1) * piece)
    copies = [pltpu.make_async_copy(combine_hbm, combine_ref, sem.at[0])]
    for k in range(shards):
        place = output_ref.at[k * capacity : (k + 1) * capacity, :]
        copies.append(pltpu.make_async_copy(blocks[k], place, sem.at[1 + k]))
    copies.append(
        pltpu.make_async_copy(here_hbm.at[:, span], here_ref, sem.at[shards + 1])
    )
    late = [pltpu.make_async_copy(kv_hbm.at[:, span], kv_ref, sem.at[shards + 2])]
    if not first:
        late.append(pltpu.make_async_copy(square_hbm, square_ref, sem.at[shards + 3]))
        late.append(pltpu.make_async_copy(cache_hbm, cache_ref, sem.at[shards + 4]))
    for copy in copies + late:
        copy.start()
    for copy in copies:
        copy.wait()
    added = jnp.dot(combine_ref[...], output_ref[...], preferred_element_type=jnp.float32)
    here_ref[...] = (here_ref[...].astype(jnp.float32) + added).astype(jnp.bfloat16)
    rows = outs[0].shape[0]
    mine = here_ref[pl.ds(pl.multiple_of(own_ref[0] * rows, rows), rows), :]
    if last:
        for j in range(stage):
            outs[0][:, j * piece : (j + 1) * piece] = before[j][...]
        outs[0][:, span] = mine
    else:
        outs[0][...] = mine
    wide = here_ref[...].astype(jnp.float32)
    scaled = (wide * gain_ref[:, span].astype(jnp.float32)).astype(jnp.bfloat16)
    square = jnp.sum(wide * wide, axis=-1, keepdims=True)
    for copy in late:
        copy.wait()
    cache = lax.dot_general(
        kv_ref[...], scaled, (((1,), (1,)), ((), ())), preferred_element_type=jnp.float32
    )
    if not first:
        cache = cache + cache_ref[...]
        square = square + square_ref[...]
    square = jnp.broadcast_to(square, square_ref.shape)
    if last:
        scale = lax.rsqrt(square / (piece * stages) + 1e-06)
        outs[1][...] = (cache * jnp.transpose(scale)[0:1, :]).astype(jnp.bfloat16)
    else:
        outs[1][...] = square
        outs[2][...] = cache


def finish(stage, stages, blocks, combine, here, own, gain, kv_matrix, rows, state):
    (total, width), (capacity, piece) = here.shape, blocks[0].shape
    heads = kv_matrix.shape[0]
    vmem = pl.BlockSpec(memory_space=pltpu.VMEM)
    hbm = pl.BlockSpec(memory_space=pl.ANY)
    shards = len(blocks)
    if stage == stages - 1:
        shapes = [((rows, width), jnp.bfloat16), ((heads, total), jnp.bfloat16)]
    else:
        shapes = [
            ((rows, piece), jnp.bfloat16),
            ((total, 128), jnp.float32),
            ((heads, total), jnp.float32),
        ]
    specs = [pl.BlockSpec(memory_space=pltpu.SMEM), hbm, hbm, vmem, hbm]
    specs += [hbm] * shards + [hbm] * min(len(state), 2) + [vmem] * max(len(state) - 2, 0)
    return pl.pallas_call(
        functools.partial(finish_body, stage, stages, shards),
        in_specs=specs,
        out_specs=[vmem] * len(shapes),
        out_shape=[jax.ShapeDtypeStruct(*shape) for shape in shapes],
        scratch_shapes=[
            pltpu.VMEM(combine.shape, jnp.bfloat16),
            pltpu.VMEM((total, piece), jnp.bfloat16),
            pltpu.VMEM((heads, piece), jnp.bfloat16),
            pltpu.VMEM((shards * capacity, piece), jnp.bfloat16),
            pltpu.VMEM((total, 128), jnp.float32),
            pltpu.VMEM((heads, total), jnp.float32),
            pltpu.SemaphoreType.DMA((shards + 5,)),
        ],
        compiler_params=pltpu.CompilerParams(vmem_limit_bytes=28 * 1024 * 1024),
        name="finish",
    )(own.reshape(1), combine, here, gain.reshape(1, width), kv_matrix, *blocks, *state)


def ffn_body(count, tile, pieces, *refs):
    inputs, weights = refs[:count], refs[count : count + 3]
    outputs = refs[count + 3 : count + 3 + sum(pieces)]
    rest = refs[count + 3 + sum(pieces) :]
    held, (rows_ref, acc_ref, sem) = rest[:3], rest[3:]
    size, width = inputs[0].shape
    steps = weights[0].shape[1] // tile
    loads = []
    for i in range(steps):
        span = slice(i * tile, (i + 1) * tile)
        places = [(slice(None), span), (slice(None), span), (span, slice(None))]
        loads.append(
            [
                pltpu.make_async_copy(
                    weights[k].at[place], held[k].at[place], sem.at[3 * i + k]
                )
                for k, place in enumerate(places)
            ]
        )
    ahead = min(2, steps)
    for copy in sum(loads[:ahead], []):
        copy.start()
    for i in range(count):
        rows_ref[i * size : (i + 1) * size, :] = inputs[i][...]
    for i in range(steps):
        span = slice(i * tile, (i + 1) * tile)
        for copy in loads[i]:
            copy.wait()
        for copy in loads[i + ahead] if i + ahead < steps else []:
            copy.start()
        rows = rows_ref[...]
        gate = jnp.dot(rows, held[0][:, span], preferred_element_type=jnp.float32)
        up = jnp.dot(rows, held[1][:, span], preferred_element_type=jnp.float32)
        hidden = (jax.nn.gelu(gate, approximate=True) * up).astype(jnp.bfloat16)
        part = jnp.dot(hidden, held[2][span, :], preferred_element_type=jnp.float32)
        if i > 0:
            part = acc_ref[...] + part
        if i < steps - 1:
            acc_ref[...] = part
    at = 0
    for i in range(count):
        piece = width // pieces[i]
        for j in range(pieces[i]):
            block = part[i * size : (i + 1) * size, j * piece : (j + 1) * piece]
            outputs[at][...] = block.astype(jnp.bfloat16)
            at += 1


def ffn(inputs, weights, pieces):
    count, (size, width) = len(inputs), inputs[0].shape
    hidden = weights[0].shape[1]
    tile = 256 if hidden % 256 == 0 else 128
    vmem = pl.BlockSpec(memory_space=pltpu.VMEM)
    shapes = [
        jax.ShapeDtypeStruct((size, width // parts), jnp.bfloat16)
        for parts in pieces
        for _ in range(parts)
    ]
    flat = pl.pallas_call(
        functools.partial(ffn_body, count, tile, pieces),
        in_specs=[vmem] * count + [pl.BlockSpec(memory_space=pltpu.HBM)] * 3,
        out_specs=[vmem] * len(shapes),
        out_shape=shapes,
        scratch_shapes=[
            pltpu.VMEM((width, hidden), jnp.bfloat16),
            pltpu.VMEM((width, hidden), jnp.bfloat16),
            pltpu.VMEM((hidden, width), jnp.bfloat16),
            pltpu.VMEM((count * size, width), jnp.bfloat16),
            pltpu.VMEM((count * size, width), jnp.float32),
            pltpu.SemaphoreType.DMA((3 * (hidden // tile),)),
        ],
        compiler_params=pltpu.CompilerParams(vmem_limit_bytes=50 * 1024 * 1024),
        cost_estimate=pl.CostEstimate(
            flops=6 * count * size * width * hidden,
            bytes_accessed=6 * width * hidden + 4 * count * size * width,
            transcendentals=count * size * hidden,
        ),
        name="ffn",
    )(*inputs, *weights)
    flat = list(flat)
    return [[flat.pop(0) for _ in range(parts)] for parts in pieces]


def local(
    tokens,
    norm_gain,
    router_weight,
    gate_weight,
    up_weight,
    down_weight,
    expert_picks,
    final_gain,
    kv_weight,
):
    shards = lax.axis_size("expert")
    groups = lax.axis_size("dp")
    own = lax.axis_index("expert")
    tok_rows, width = tokens.shape
    group_rows = shards * tok_rows
    order = jnp.arange(shards, dtype=jnp.int32) ^ own
    base = order * tok_rows
    picks = expert_picks[0][order]
    weights = (gate_weight[0], up_weight[0], down_weight[0])

    dense = fits([tokens] * shards)
    own_picks = lax.dynamic_slice_in_dim(expert_picks[0], own, 1, 0)
    far = {
        mask: (shuffle(tokens, "dp", mask), shuffle(own_picks, "dp", mask))
        for mask in range(groups - 1, 1, -1)
        if dense
    }
    blocks = plane_gather(tokens)
    inputs = {0: select(blocks, own_picks, base, norm_gain)}
    for mask in range(1, groups):
        if mask not in far:
            inputs[mask] = shuffle(inputs[0], "dp", mask)
    for mask, (spread, rows) in far.items():
        gathered = plane_gather(spread)
        inputs[mask] = select(gathered, rows, base, norm_gain)
    combine, here = prepare(
        blocks, picks, base, own, norm_gain, router_weight[:, order]
    )

    stages = 2 if dense else 1
    piece = width // stages
    split = lambda mask: stages if mask in (1, 2) and dense else 1
    parts = {}
    sequence = [0] + list(range(groups - 1, 0, -1))
    half = max(groups // 2, 1)
    for start in range(0, groups, half):
        batch = sequence[start : start + half]
        result = ffn([inputs[m] for m in batch], weights, [split(m) for m in batch])
        parts.update(zip(batch, result))
    last = groups - 1
    close = lambda i: groups <= 2 or abs(i - (i ^ last)) == 1
    if groups > 2:
        passed = [
            shuffle(value, "dp", 1, lambda i: not close(i))
            for value in parts[last]
        ]
        passed = jnp.concatenate(passed, axis=1) if len(passed) > 1 else passed[0]
        size = passed.shape[1] // len(parts[last - 1])
        parts[last - 1] = [
            (value.astype(jnp.float32) + passed[:, j * size : (j + 1) * size]).astype(
                jnp.bfloat16
            )
            for j, value in enumerate(parts[last - 1])
        ]
    received = {
        mask: [
            shuffle(value, "dp", mask, close if mask == last else lambda i: True)
            for value in parts[mask]
        ]
        for mask in range(1, groups)
    }
    received[0] = parts[0]
    kv_matrix = kv_weight.reshape(width, -1).T
    state = []
    for stage in range(stages):
        total = 0.0
        for mask in sequence:
            values = received[mask]
            value = values[stage] if len(values) == stages else values[0]
            if stage > 0:
                value, _ = lax.optimization_barrier((value, summed))
            if value.shape[1] != piece:
                value = value[:, stage * piece : (stage + 1) * piece]
            total += value.astype(jnp.float32)
        summed = total.astype(jnp.bfloat16)
        returned = plane_gather(summed)
        if not dense:
            moe_out, kv_rows = plain_finish(
                returned, combine, here, own, final_gain, kv_matrix, tok_rows
            )
            continue
        result = finish(
            stage, stages, returned, combine, here, own, final_gain, kv_matrix, tok_rows, state
        )
        if stage == stages - 1:
            moe_out, kv_rows = result
        else:
            state = [result[1], result[2]] + state[2:] + [result[0]]
    kv_cache = kv_rows.T.reshape((group_rows,) + kv_weight.shape[1:])
    return (moe_out, kv_cache)


def solution(mesh):
    in_specs = (
        P(("dp", "expert"), None),
        P(),
        P(),
        P("expert", None, "dp"),
        P("expert", None, "dp"),
        P("expert", "dp", None),
        P("dp", None, None),
        P(),
        P(None, "expert", None, None, None),
    )
    out_specs = (P(("dp", "expert"), None), P("dp", "expert", None, None, None))

    return jax.shard_map(local, mesh=mesh, in_specs=in_specs, out_specs=out_specs, check_vma=False)
```

```python
import functools

import jax
import jax.numpy as jnp
from jax import lax
from jax.experimental import pallas as pl
from jax.experimental.pallas import tpu as pltpu
from jax.sharding import PartitionSpec as P


def shuffle(value, axis, mask, keep=lambda i: True):
    size = lax.axis_size(axis)
    return lax.ppermute(value, axis, [(i, i ^ mask) for i in range(size) if keep(i)])


def plane_gather(value):
    size = lax.axis_size("expert")
    blocks = {0: value}
    for mask in range(2, size, 2):
        blocks[mask] = shuffle(value, "expert", mask)
    for mask in range(0, size, 2):
        blocks[mask + 1] = shuffle(blocks[mask], "expert", 1)
    return [blocks[mask] for mask in range(size)]


def pick_rows(base_ref, picks, gain, blocks):
    rows, capacity = blocks[0].shape[0], picks.shape[1]
    column = lax.broadcasted_iota(jnp.int32, (rows, capacity), 0)
    hits = jnp.concatenate(
        [
            (column + base_ref[k] == picks).astype(jnp.bfloat16)
            for k in range(len(blocks))
        ],
        axis=0,
    )
    values = jnp.concatenate([block[...] for block in blocks], axis=0)
    chosen = lax.dot_general(
        hits, values, (((0,), (0,)), ((), ())), preferred_element_type=jnp.float32
    )
    scale = lax.rsqrt(jnp.mean(chosen * chosen, axis=-1, keepdims=True) + 1e-06)
    return (chosen * scale * gain.astype(jnp.float32)).astype(jnp.bfloat16)


def select_body(base_ref, picks_ref, gain_ref, *refs):
    refs[-1][...] = pick_rows(base_ref, picks_ref[...], gain_ref[...], refs[:-1])


def fits(blocks):
    return len(blocks) * blocks[0].size <= 2 * 1024 * 1024


def plain_normalize(wide, gain):
    scale = lax.rsqrt(jnp.mean(wide * wide, axis=-1, keepdims=True) + 1e-06)
    return (wide * scale * gain.astype(jnp.float32)).astype(jnp.bfloat16)


def token_ids(base, rows):
    return (base[:, None] + jnp.arange(rows, dtype=jnp.int32)[None, :]).reshape(-1)


def plain_select(blocks, picks, base, gain):
    ids = token_ids(base, blocks[0].shape[0])
    hits = (picks.reshape(-1, 1) == ids[None, :]).astype(jnp.bfloat16)
    values = jnp.concatenate(blocks, axis=0)
    return plain_normalize(jnp.dot(hits, values, preferred_element_type=jnp.float32), gain)


def plain_prepare(blocks, picks, base, gain, router):
    rows = blocks[0].shape[0]
    all_ids = jnp.arange(len(blocks) * rows, dtype=jnp.int32)
    place = (all_ids[:, None] == token_ids(base, rows)[None, :]).astype(jnp.bfloat16)
    values = jnp.concatenate(blocks, axis=0)
    here = jnp.dot(place, values, preferred_element_type=jnp.float32)
    probs = jax.nn.sigmoid(
        jnp.dot(plain_normalize(here, gain), router, preferred_element_type=jnp.float32)
    )
    hits = all_ids[:, None, None] == picks[None, :, :]
    combine = jnp.where(hits, probs[:, :, None], 0.0).astype(jnp.bfloat16)
    return combine.reshape(all_ids.shape[0], -1), here.astype(jnp.bfloat16)


def plain_finish(blocks, combine, here, own, gain, kv_matrix, rows):
    outputs = jnp.concatenate(blocks, axis=0)
    added = jnp.dot(combine, outputs, preferred_element_type=jnp.float32)
    moe = (here.astype(jnp.float32) + added).astype(jnp.bfloat16)
    encoded = plain_normalize(moe.astype(jnp.float32), gain)
    cache = lax.dot_general(
        kv_matrix, encoded, (((1,), (1,)), ((), ())), preferred_element_type=jnp.float32
    ).astype(jnp.bfloat16)
    return lax.dynamic_slice_in_dim(moe, own * rows, rows, 0), cache


def select(blocks, picks, base, gain):
    if not fits(blocks):
        return plain_select(blocks, picks, base, gain)
    capacity, width = picks.shape[-1], blocks[0].shape[1]
    vmem = pl.BlockSpec(memory_space=pltpu.VMEM)
    return pl.pallas_call(
        select_body,
        in_specs=[pl.BlockSpec(memory_space=pltpu.SMEM)] + [vmem] * (2 + len(blocks)),
        out_specs=vmem,
        out_shape=jax.ShapeDtypeStruct((capacity, width), jnp.bfloat16),
        compiler_params=pltpu.CompilerParams(vmem_limit_bytes=12 * 1024 * 1024),
        name="select",
    )(base, picks.reshape(1, capacity), gain.reshape(1, width), *blocks)


def prepare_body(base_ref, own_ref, picks_ref, gain_ref, router_ref, *refs):
    blocks, (combine_ref, here_ref) = refs[:-2], refs[-2:]
    rows, _ = blocks[0].shape
    shards = len(blocks)
    capacity = picks_ref.shape[1]
    gain = gain_ref[...].astype(jnp.float32)
    for k in range(shards):
        wide = blocks[k][...].astype(jnp.float32)
        scale = lax.rsqrt(jnp.mean(wide * wide, axis=-1, keepdims=True) + 1e-06)
        normed = (wide * scale * gain).astype(jnp.bfloat16)
        logits = jnp.dot(normed, router_ref[...], preferred_element_type=jnp.float32)
        probs = jax.nn.sigmoid(logits)
        start = pl.multiple_of(base_ref[k], rows)
        here_ref[pl.ds(start, rows), :] = blocks[k][...]
        ids = lax.broadcasted_iota(jnp.int32, (rows, capacity), 0) + start
        for j in range(shards):
            hit = ids == picks_ref[j : j + 1, :]
            combine_ref[pl.ds(start, rows), j * capacity : (j + 1) * capacity] = (
                jnp.where(hit, probs[:, j : j + 1], 0.0).astype(jnp.bfloat16)
            )


def prepare(blocks, picks, base, own, gain, router):
    if not fits(blocks):
        return plain_prepare(blocks, picks, base, gain, router)
    shards, (rows, width) = len(blocks), blocks[0].shape
    capacity = picks.shape[1]
    vmem = pl.BlockSpec(memory_space=pltpu.VMEM)
    smem = pl.BlockSpec(memory_space=pltpu.SMEM)
    return pl.pallas_call(
        prepare_body,
        in_specs=[smem, smem] + [vmem] * (3 + shards),
        out_specs=[vmem, vmem],
        out_shape=[
            jax.ShapeDtypeStruct((shards * rows, shards * capacity), jnp.bfloat16),
            jax.ShapeDtypeStruct((shards * rows, width), jnp.bfloat16),
        ],
        compiler_params=pltpu.CompilerParams(vmem_limit_bytes=24 * 1024 * 1024),
        name="prepare",
    )(base, own.reshape(1), picks, gain.reshape(1, width), router, *blocks)


def finish_body(stage, stages, start, width, shards, *refs):
    own_ref, combine_ref, here_ref, gain_ref, kv_ref = refs[:5]
    blocks, refs = refs[5 : 5 + shards], refs[5 + shards :]
    first, last = stage == 0, stage == stages - 1
    if not first:
        (square_ref, cache_ref, *before), refs = refs[: 2 + stage], refs[2 + stage :]
    outs, moe_ref = refs[:-1], refs[-1]
    piece = blocks[0].shape[1]
    span = slice(start, start + piece)
    outputs = jnp.concatenate([block[...] for block in blocks], axis=0)
    added = jnp.dot(combine_ref[...], outputs, preferred_element_type=jnp.float32)
    moe_ref[...] = (here_ref[:, span].astype(jnp.float32) + added).astype(jnp.bfloat16)
    rows = outs[0].shape[0]
    mine = moe_ref[pl.ds(pl.multiple_of(own_ref[0] * rows, rows), rows), :]
    if last:
        at = 0
        for value in before:
            outs[0][:, at : at + value.shape[1]] = value[...]
            at += value.shape[1]
        outs[0][:, span] = mine
    else:
        outs[0][...] = mine
    wide = moe_ref[...].astype(jnp.float32)
    scaled = (wide * gain_ref[:, span].astype(jnp.float32)).astype(jnp.bfloat16)
    square = jnp.sum(wide * wide, axis=-1, keepdims=True)
    cache = lax.dot_general(
        kv_ref[:, span], scaled, (((1,), (1,)), ((), ())), preferred_element_type=jnp.float32
    )
    if not first:
        cache = cache + cache_ref[...]
        square = square + square_ref[...]
    square = jnp.broadcast_to(square, (square.shape[0], 128))
    if last:
        scale = lax.rsqrt(square / width + 1e-06)
        outs[1][...] = (cache * jnp.transpose(scale)[0:1, :]).astype(jnp.bfloat16)
    else:
        outs[1][...] = square
        outs[2][...] = cache


def finish(stage, stages, start, blocks, combine, here, own, gain, kv_matrix, rows, state):
    (total, width), piece = here.shape, blocks[0].shape[1]
    heads = kv_matrix.shape[0]
    vmem = pl.BlockSpec(memory_space=pltpu.VMEM)
    shards = len(blocks)
    if stage == stages - 1:
        shapes = [((rows, width), jnp.bfloat16), ((heads, total), jnp.bfloat16)]
    else:
        shapes = [
            ((rows, piece), jnp.bfloat16),
            ((total, 128), jnp.float32),
            ((heads, total), jnp.float32),
        ]
    return pl.pallas_call(
        functools.partial(finish_body, stage, stages, start, width, shards),
        in_specs=[pl.BlockSpec(memory_space=pltpu.SMEM)]
        + [vmem] * (4 + shards + len(state)),
        out_specs=[vmem] * len(shapes),
        out_shape=[jax.ShapeDtypeStruct(*shape) for shape in shapes],
        scratch_shapes=[pltpu.VMEM((total, piece), jnp.bfloat16)],
        compiler_params=pltpu.CompilerParams(vmem_limit_bytes=28 * 1024 * 1024),
        name="finish",
    )(own.reshape(1), combine, here, gain.reshape(1, width), kv_matrix, *blocks, *state)


def ffn_body(layout, tile, widths, base_ref, gain_ref, *refs):
    total = sum(layout)
    inputs, weights = refs[:total], refs[total : total + 3]
    ends = total + 3 + sum(len(parts) for parts in widths)
    outputs, rest = refs[total + 3 : ends], refs[ends:]
    held, (rows_ref, acc_ref, sem) = rest[:3], rest[3:]
    size = rows_ref.shape[0] // len(layout)
    steps = weights[0].shape[1] // tile
    loads = []
    for i in range(steps):
        span = slice(i * tile, (i + 1) * tile)
        places = [(slice(None), span), (slice(None), span), (span, slice(None))]
        loads.append(
            [
                pltpu.make_async_copy(
                    weights[k].at[place], held[k].at[place], sem.at[3 * i + k]
                )
                for k, place in enumerate(places)
            ]
        )
    ahead = min(3, steps)
    for copy in sum(loads[:ahead], []):
        copy.start()
    at = 0
    for i, count in enumerate(layout):
        span = slice(i * size, (i + 1) * size)
        if count == 1:
            rows_ref[span, :] = inputs[at][...]
        else:
            rows_ref[span, :] = pick_rows(
                base_ref, inputs[at][...], gain_ref[...], inputs[at + 1 : at + count]
            )
        at += count
    for i in range(steps):
        span = slice(i * tile, (i + 1) * tile)
        for copy in loads[i]:
            copy.wait()
        for copy in loads[i + ahead] if i + ahead < steps else []:
            copy.start()
        rows = rows_ref[...]
        gate = jnp.dot(rows, held[0][:, span], preferred_element_type=jnp.float32)
        up = jnp.dot(rows, held[1][:, span], preferred_element_type=jnp.float32)
        hidden = (jax.nn.gelu(gate, approximate=True) * up).astype(jnp.bfloat16)
        part = jnp.dot(hidden, held[2][span, :], preferred_element_type=jnp.float32)
        if i > 0:
            part = acc_ref[...] + part
        if i < steps - 1:
            acc_ref[...] = part
    at = 0
    for i, parts in enumerate(widths):
        start = 0
        for piece in parts:
            block = part[i * size : (i + 1) * size, start : start + piece]
            outputs[at][...] = block.astype(jnp.bfloat16)
            at, start = at + 1, start + piece


def ffn(inputs, weights, widths, base, gain):
    width, hidden = weights[0].shape
    layout = [len(item) for item in inputs]
    size = next(i[0].shape[0] if len(i) == 1 else i[0].shape[1] for i in inputs)
    count = len(inputs)
    tile = 256 if hidden % 256 == 0 else 128
    vmem = pl.BlockSpec(memory_space=pltpu.VMEM)
    shapes = [
        jax.ShapeDtypeStruct((size, piece), jnp.bfloat16)
        for parts in widths
        for piece in parts
    ]
    flat = pl.pallas_call(
        functools.partial(ffn_body, layout, tile, widths),
        in_specs=[pl.BlockSpec(memory_space=pltpu.SMEM)]
        + [vmem] * (1 + sum(layout))
        + [pl.BlockSpec(memory_space=pltpu.HBM)] * 3,
        out_specs=[vmem] * len(shapes),
        out_shape=shapes,
        scratch_shapes=[
            pltpu.VMEM((width, hidden), jnp.bfloat16),
            pltpu.VMEM((width, hidden), jnp.bfloat16),
            pltpu.VMEM((hidden, width), jnp.bfloat16),
            pltpu.VMEM((count * size, width), jnp.bfloat16),
            pltpu.VMEM((count * size, width), jnp.float32),
            pltpu.SemaphoreType.DMA((3 * (hidden // tile),)),
        ],
        compiler_params=pltpu.CompilerParams(vmem_limit_bytes=50 * 1024 * 1024),
        cost_estimate=pl.CostEstimate(
            flops=6 * count * size * width * hidden,
            bytes_accessed=6 * width * hidden + 4 * count * size * width,
            transcendentals=count * size * hidden,
        ),
        name="ffn",
    )(base, gain.reshape(1, width), *sum(map(list, inputs), []), *weights)
    flat = list(flat)
    return [[flat.pop(0) for _ in parts] for parts in widths]


def local(
    tokens,
    norm_gain,
    router_weight,
    gate_weight,
    up_weight,
    down_weight,
    expert_picks,
    final_gain,
    kv_weight,
):
    shards = lax.axis_size("expert")
    groups = lax.axis_size("dp")
    own = lax.axis_index("expert")
    tok_rows, width = tokens.shape
    group_rows = shards * tok_rows
    order = jnp.arange(shards, dtype=jnp.int32) ^ own
    base = order * tok_rows
    picks = expert_picks[0][order]
    weights = (gate_weight[0], up_weight[0], down_weight[0])

    dense = fits([tokens] * shards)
    own_picks = lax.dynamic_slice_in_dim(expert_picks[0], own, 1, 0)
    far = {
        mask: (shuffle(tokens, "dp", mask), shuffle(own_picks, "dp", mask))
        for mask in range(groups - 1, 1, -1)
        if dense
    }
    blocks = plane_gather(tokens)
    inputs = {0: select(blocks, own_picks, base, norm_gain)}
    for mask in range(1, groups):
        if mask not in far:
            inputs[mask] = shuffle(inputs[0], "dp", mask)
    inputs = {mask: (value,) for mask, value in inputs.items()}
    for mask, (spread, rows) in far.items():
        inputs[mask] = (rows, *plane_gather(spread))
    combine, here = prepare(
        blocks, picks, base, own, norm_gain, router_weight[:, order]
    )

    wide_first = width * 9 // 16
    pieces = [wide_first, width - wide_first] if dense else [width]
    stages = len(pieces)
    split = lambda mask: pieces if mask in (1, 2) else [width]
    parts = {}
    sequence = [0] + list(range(groups - 1, 0, -1))
    half = max(groups // 2, 1)
    for start in range(0, groups, half):
        batch = sequence[start : start + half]
        result = ffn(
            [inputs[m] for m in batch],
            weights,
            [split(m) for m in batch],
            base,
            norm_gain,
        )
        parts.update(zip(batch, result))
    last = groups - 1
    close = lambda i: groups <= 2 or abs(i - (i ^ last)) == 1
    if groups > 2:
        passed = [
            shuffle(value, "dp", 1, lambda i: not close(i))
            for value in parts[last]
        ]
        passed = jnp.concatenate(passed, axis=1) if len(passed) > 1 else passed[0]
        start, joined = 0, []
        for value in parts[last - 1]:
            extra = passed[:, start : start + value.shape[1]]
            joined.append((value.astype(jnp.float32) + extra).astype(jnp.bfloat16))
            start += value.shape[1]
        parts[last - 1] = joined
    received = {
        mask: [
            shuffle(value, "dp", mask, close if mask == last else lambda i: True)
            for value in parts[mask]
        ]
        for mask in range(1, groups)
    }
    received[0] = parts[0]
    kv_matrix = kv_weight.reshape(width, -1).T
    state, start = [], 0
    for stage, piece in enumerate(pieces):
        total = 0.0
        for mask in sequence:
            values = received[mask]
            value = values[stage] if len(values) == stages else values[0]
            if stage > 0:
                value, _ = lax.optimization_barrier((value, summed))
            if value.shape[1] != piece:
                value = value[:, start : start + piece]
            total += value.astype(jnp.float32)
        summed = total.astype(jnp.bfloat16)
        returned = plane_gather(summed)
        if not dense:
            moe_out, kv_rows = plain_finish(
                returned, combine, here, own, final_gain, kv_matrix, tok_rows
            )
            continue
        result = finish(
            stage, stages, start, returned, combine, here, own, final_gain, kv_matrix, tok_rows, state
        )
        if stage == stages - 1:
            moe_out, kv_rows = result
        else:
            state = [result[1], result[2]] + state[2:] + [result[0]]
        start += piece
    kv_cache = kv_rows.T.reshape((group_rows,) + kv_weight.shape[1:])
    return (moe_out, kv_cache)


def solution(mesh):
    in_specs = (
        P(("dp", "expert"), None),
        P(),
        P(),
        P("expert", None, "dp"),
        P("expert", None, "dp"),
        P("expert", "dp", None),
        P("dp", None, None),
        P(),
        P(None, "expert", None, None, None),
    )
    out_specs = (P(("dp", "expert"), None), P("dp", "expert", None, None, None))

    return jax.shard_map(local, mesh=mesh, in_specs=in_specs, out_specs=out_specs, check_vma=False)
```
